8 devices in a mesh: rep: 1 (over z), dp: 8 (over x, y, core).
Axes of the slice: x: 2, y: 2, z: 1, core: 2. Of those that a mesh axis runs over, the one named last changes fastest.
Arguments:
- a: bfloat16 [8, 4, 4096, 1024], P(('rep', 'dp'))
- g: bfloat16 [8, 4, 4096, 3328], P(('rep', 'dp'))
Outputs:
- output: bfloat16 [4, 1024, 3328], P('rep')
All inputs are finite; a program needn't handle non-finite values.
Results may differ from the reference program's by a relative error of at most 0.012.
Values are sent between devices in bfloat16 or wider.
A program may use at most 2 GiB of HBM per device.

```python
import jax
import jax.numpy as jnp
from jax import lax

DEVICES = 8
MATRICES = 4
TOKENS = 4096
D = 1024
FF = 3328


def setup_inputs(seed: int = 0, part: int = 0) -> dict:
    ka, kg, ks = (jax.random.fold_in(k, part) for k in jax.random.split(jax.random.key(seed), 3))
    size = 2.0 ** jax.random.uniform(ks, (DEVICES, MATRICES, 1, 1), jnp.float32, -1.0, 1.0)
    a = jax.random.normal(ka, (DEVICES, MATRICES, TOKENS, D), jnp.float32)
    g = size * jax.random.normal(kg, (DEVICES, MATRICES, TOKENS, FF), jnp.float32) * (DEVICES * TOKENS) ** -0.5
    return {"a": a.astype(jnp.bfloat16), "g": g.astype(jnp.bfloat16)}


def reference(a, g):
    def take(so_far, one):
        return so_far + jnp.einsum("ntd,ntf->ndf", *one, preferred_element_type=jnp.float32), None

    return lax.scan(take, jnp.zeros((MATRICES, D, FF), jnp.float32), (a, g))[0].astype(jnp.bfloat16)
```

```python
import functools
import jax
import jax.numpy as jnp
from jax import lax
from jax.experimental import pallas as pl
from jax.experimental.pallas import tpu as pltpu
from jax.sharding import PartitionSpec as P

MESH = pl.DeviceIdType.MESH
W = 256
KC = 512
AG_START, AG_EVERY = 8, 4


def kernel(a_ref, g_ref, t_ref, at, a_in, g_in, mine, d2d_out, d2d_got, rs1_out, rs1_got, keep1,
           rs2_out, rs2_got, keep2, fin,
           a_sem, g_sem, d2d_s, d2d_r, rs1_s, rs1_r, rs2_s, rs2_r, ag1_r, ag2a_r, ag2b_r, sib_r, ag_s, loc_s):
    mats, tokens, d = a_ref.shape[1:]
    ff = g_ref.shape[3]
    nb = ff // W
    rounds = mats * nb
    half_d, h, q4 = d // 2, d // 4, d // 8
    chunks = tokens // KC

    me = lax.axis_index("dp")
    x, y, c = me // 4, (me // 2) % 2, me % 2
    pa = (1 - c) * x + c * y
    pb = (1 - c) * y + c * x
    to_a = me + (1 - c) * (4 - 8 * x) + c * (2 - 4 * y)
    to_b = me + (1 - c) * (2 - 4 * y) + c * (4 - 8 * x)
    sib = me + 1 - 2 * c
    own, other = half_d * c, half_d * (1 - c)

    def at_rows(ref, start, size):
        return ref.at[pl.ds(pl.multiple_of(start, 128), size)]

    def remote(src, dst, s, r, dev):
        return pltpu.make_async_remote_copy(src_ref=src, dst_ref=dst, send_sem=s, recv_sem=r,
                                            device_id={"dp": dev}, device_id_type=MESH)

    def tile(r, start, size):
        n, j = r // nb, r % nb
        return t_ref.at[n, pl.ds(pl.multiple_of(start, 128), size), pl.ds(pl.multiple_of(j * W, W), W)]

    def g_copy(r):
        n, j = r // nb, r % nb
        return pltpu.make_async_copy(g_ref.at[0, n, :, pl.ds(pl.multiple_of(j * W, W), W)],
                                     g_in.at[r % 3], g_sem.at[r % 3])

    def a_copy(n, k):
        return pltpu.make_async_copy(a_ref.at[0, n, pl.ds(pl.multiple_of(k * KC, KC), KC)],
                                     a_in.at[k % 2], a_sem.at[k % 2])

    def turn(n, k):
        at[n % 2, :, pl.ds(pl.multiple_of(k * KC, KC), KC)] = a_in[k % 2].T

    def d2d(r):
        return remote(d2d_out.at[r % 4], d2d_got.at[r % 4], d2d_s.at[r % 4], d2d_r.at[r % 4], sib)

    def rs1(r):
        return remote(rs1_out.at[r % 8], rs1_got.at[r % 8], rs1_s.at[r % 8], rs1_r.at[r % 8], to_a)

    def rs2(r):
        return remote(rs2_out.at[r % 8], rs2_got.at[r % 8], rs2_s.at[r % 8], rs2_r.at[r % 8], to_b)

    def dot(r, rows):
        return jnp.dot(at[(r // nb) % 2, pl.ds(pl.multiple_of(rows, half_d), half_d), :], g_in[r % 3],
                       preferred_element_type=jnp.float32)

    def combine(r):
        d2d(r).wait_recv()
        lo, up = pl.multiple_of(h * (1 - pa), h), pl.multiple_of(h * pa, h)

        @pl.when(r >= 8)
        def _():
            rs1(r - 8).wait_send()

        rs1_out[r % 8] = (mine[pl.ds(lo, h)] + d2d_got[r % 4, pl.ds(lo, h)].astype(jnp.float32)).astype(jnp.bfloat16)
        rs1(r).start()
        keep1[r % 4] = mine[pl.ds(up, h)] + d2d_got[r % 4, pl.ds(up, h)].astype(jnp.float32)

    def stage2(r):
        rs1(r).wait_recv()
        lo, up = pl.multiple_of(q4 * (1 - pb), q4), pl.multiple_of(q4 * pb, q4)

        @pl.when(r >= 8)
        def _():
            rs2(r - 8).wait_send()

        rs2_out[r % 8] = (keep1[r % 4, pl.ds(lo, q4)] + rs1_got[r % 8, pl.ds(lo, q4)].astype(jnp.float32)).astype(jnp.bfloat16)
        rs2(r).start()
        keep2[r % 4] = keep1[r % 4, pl.ds(up, q4)] + rs1_got[r % 8, pl.ds(up, q4)].astype(jnp.float32)

    def stage3(r):
        rs2(r).wait_recv()
        fin[r] = (keep2[r % 4] + rs2_got[r % 8].astype(jnp.float32)).astype(jnp.bfloat16)

    def quarter(p, q):
        return own + h * p + q4 * q

    def spread1(r):
        dst = tile(r, quarter(pa, pb), q4)
        remote(fin.at[r], dst, ag_s, ag1_r.at[r], to_b).start()
        remote(fin.at[r], dst, ag_s, ag2a_r.at[r], to_a).start()
        remote(fin.at[r], dst, ag_s, sib_r, sib).start()
        pltpu.make_async_copy(fin.at[r], dst, loc_s).start()

    def spread2(r):
        src = tile(r, quarter(pa, 1 - pb), q4)
        remote(fin.at[r], src, ag_s, ag1_r.at[r], to_b).wait_recv()
        remote(src, src, ag_s, ag2b_r.at[r], to_a).start()
        remote(src, src, ag_s, sib_r, sib).start()

    def spread3(r):
        dst = tile(r, quarter(1 - pa, pb), q4)
        remote(fin.at[r], dst, ag_s, ag2a_r.at[r], to_a).wait_recv()
        dst = tile(r, quarter(1 - pa, 1 - pb), q4)
        remote(fin.at[r], dst, ag_s, ag2b_r.at[r], to_a).wait_recv()
        src = tile(r, own + h * (1 - pa), h)
        remote(src, src, ag_s, sib_r, sib).start()

    a_copy(0, 0).start()
    a_copy(0, 1).start()
    for r in range(2):
        g_copy(r).start()

    barrier = pltpu.get_barrier_semaphore()
    for dev in (sib, to_a, to_b):
        pl.semaphore_signal(barrier, inc=1, device_id={"dp": dev}, device_id_type=MESH)
    pl.semaphore_wait(barrier, 3)

    @pl.loop(0, chunks)
    def _(k):
        a_copy(0, k).wait()
        turn(0, k)

        @pl.when(k + 2 < chunks)
        def _():
            a_copy(0, k + 2).start()

    @pl.loop(0, rounds + 5)
    def _(r):
        n, j = r // nb, r % nb
        nxt = (n + 1 < mats)

        @pl.when(r < rounds)
        def _():
            @pl.when(nxt & (j == 0))
            def _():
                a_copy(n + 1, 0).start()
                a_copy(n + 1, 1).start()

            g_copy(r).wait()

            @pl.when(r + 2 < rounds)
            def _():
                g_copy(r + 2).start()

            @pl.when(r >= 4)
            def _():
                d2d(r - 4).wait_send()

            d2d_out[r % 4] = dot(r, other).astype(jnp.bfloat16)
            d2d(r).start()

        @pl.when((r >= 1) & (r <= rounds))
        def _():
            combine(r - 1)

        @pl.when(r < rounds)
        def _():
            mine[...] = dot(r, own)

        @pl.when((r >= 3) & (r < rounds + 3))
        def _():
            stage2(r - 3)

        @pl.when(r >= 5)
        def _():
            stage3(r - 5)

        @pl.when(nxt & (j >= 1) & (j <= chunks))
        def _():
            k = j - 1
            a_copy(n + 1, k).wait()
            turn(n + 1, k)

            @pl.when(k + 2 < chunks)
            def _():
                a_copy(n + 1, k + 2).start()

        s = (r - AG_START) // AG_EVERY

        @pl.when((r >= AG_START) & ((r - AG_START) % AG_EVERY == 0))
        def _():
            spread1(s)

            @pl.when(s >= 1)
            def _():
                spread2(s - 1)

            @pl.when(s >= 2)
            def _():
                spread3(s - 2)

    done = (rounds + 5 - AG_START + AG_EVERY - 1) // AG_EVERY

    @pl.loop(done, rounds)
    def _(s):
        spread1(s)

    @pl.loop(done - 1, rounds + 1)
    def _(s):
        @pl.when(s < rounds)
        def _():
            spread2(s)

        spread3(s - 1)

    for k in range(4):
        d2d(rounds - 4 + k).wait_send()
    for k in range(8):
        rs1(rounds - 8 + k).wait_send()
        rs2(rounds - 8 + k).wait_send()
    whole = t_ref.at[:, pl.ds(0, d - q4), :]
    remote(whole, whole, ag_s, sib_r, sib).wait_send()
    part = t_ref.at[:, pl.ds(0, half_d), :]
    remote(part, part, ag_s, sib_r, sib).wait_recv()
    mini = t_ref.at[:, pl.ds(0, q4), :]
    pltpu.make_async_copy(mini, mini, loc_s).wait()


def solution(mesh):
    def step(a, g):
        mats, tokens, d = a.shape[1:]
        ff = g.shape[3]
        rounds = mats * (ff // W)
        bf, f32 = jnp.bfloat16, jnp.float32
        dma = pltpu.SemaphoreType.DMA
        scratch = [
            pltpu.VMEM((2, d, tokens), bf),
            pltpu.VMEM((2, KC, d), bf),
            pltpu.VMEM((3, tokens, W), bf),
            pltpu.VMEM((d // 2, W), f32),
            pltpu.VMEM((4, d // 2, W), bf),
            pltpu.VMEM((4, d // 2, W), bf),
            pltpu.VMEM((8, d // 4, W), bf),
            pltpu.VMEM((8, d // 4, W), bf),
            pltpu.VMEM((4, d // 4, W), f32),
            pltpu.VMEM((8, d // 8, W), bf),
            pltpu.VMEM((8, d // 8, W), bf),
            pltpu.VMEM((4, d // 8, W), f32),
            pltpu.VMEM((rounds, d // 8, W), bf),
            dma((2,)), dma((3,)), dma((4,)), dma((4,)), dma((8,)), dma((8,)), dma((8,)), dma((8,)),
            dma((rounds,)), dma((rounds,)), dma((rounds,)), dma, dma, dma,
        ]
        return pl.pallas_call(
            kernel,
            out_shape=jax.ShapeDtypeStruct((mats, d, ff), bf),
            in_specs=[pl.BlockSpec(memory_space=pl.ANY)] * 2,
            out_specs=pl.BlockSpec(memory_space=pl.ANY),
            scratch_shapes=scratch,
            compiler_params=pltpu.CompilerParams(collective_id=0, has_side_effects=True, vmem_limit_bytes=60 << 20),
            name="sums",
        )(a, g)

    return jax.shard_map(step, mesh=mesh, in_specs=(P(("rep", "dp")), P(("rep", "dp"))), out_specs=P("rep"),
                         check_vma=False)
```

```python
import jax
import jax.numpy as jnp
from jax import lax
from jax.experimental import pallas as pl
from jax.experimental.pallas import tpu as pltpu
from jax.sharding import PartitionSpec as P

MESH = pl.DeviceIdType.MESH
W = 256
LAG1, LAG2, LAG3 = 1, 3, 5
AG_START, AG_EVERY = 7, 1


def kernel(a_ref, g_ref, t_ref, a_in, g_in, mine, d2d_out, d2d_got, rs1_out, rs1_got, keep1,
           rs2_out, rs2_got, keep2,
           a_sem, g_sem, d2d_s, d2d_r, rs1_s, rs1_r, rs2_s, rs2_r, ag1_r, ag2a_r, ag2b_r, sib_r, ag_s):
    mats, tokens, d = a_ref.shape[1:]
    ff = g_ref.shape[3]
    nb = ff // W
    rounds = mats * nb
    half_d, h, q4 = d // 2, d // 4, d // 8
    f32, bf = jnp.float32, jnp.bfloat16

    me = lax.axis_index("dp")
    x, y, c = me // 4, (me // 2) % 2, me % 2
    pa = (1 - c) * x + c * y
    pb = (1 - c) * y + c * x
    to_a = me + (1 - c) * (4 - 8 * x) + c * (2 - 4 * y)
    to_b = me + (1 - c) * (2 - 4 * y) + c * (4 - 8 * x)
    sib = me + 1 - 2 * c
    own, other = half_d * c, half_d * (1 - c)

    def remote(src, dst, s, r, dev):
        return pltpu.make_async_remote_copy(src_ref=src, dst_ref=dst, send_sem=s, recv_sem=r,
                                            device_id={"dp": dev}, device_id_type=MESH)

    def cut(r, start, size):
        return r // nb, pl.ds(pl.multiple_of(start, 128), size), pl.ds(pl.multiple_of((r % nb) * W, W), W)

    def tile(r, start, size):
        return t_ref.at[cut(r, start, size)]

    def g_copy(r):
        return pltpu.make_async_copy(g_ref.at[0, r // nb, :, pl.ds(pl.multiple_of((r % nb) * W, W), W)],
                                     g_in.at[r % 3], g_sem.at[r % 3])

    def a_copy(n, i):
        cols = pl.ds(half_d * i, half_d)
        return pltpu.make_async_copy(a_ref.at[0, n, :, cols], a_in.at[n % 2, i], a_sem.at[n % 2, i])

    def a_side(n, side):
        cols = pl.ds(pl.multiple_of(side, half_d), half_d)
        return pltpu.make_async_copy(a_ref.at[0, n, :, cols], a_in.at[n % 2, side // half_d],
                                     a_sem.at[n % 2, side // half_d])

    def d2d(r):
        return remote(d2d_out.at[r % 4], d2d_got.at[r % 4], d2d_s.at[r % 4], d2d_r.at[r % 4], sib)

    def rs1(r):
        return remote(rs1_out.at[r % 8], rs1_got.at[r % 8], rs1_s.at[r % 8], rs1_r.at[r % 8], to_a)

    def rs2(r):
        return remote(rs2_out.at[r % 8], rs2_got.at[r % 8], rs2_s.at[r % 8], rs2_r.at[r % 8], to_b)

    def dot(r, side):
        return lax.dot_general(a_in[(r // nb) % 2, side // half_d], g_in[r % 3],
                               (((0,), (0,)), ((), ())), preferred_element_type=f32)

    def combine(r):
        lo, up = pl.multiple_of(h * (1 - pa), h), pl.multiple_of(h * pa, h)
        rs1_out[r % 8] = (mine[r % 2, pl.ds(lo, h)] + d2d_got[r % 4, pl.ds(lo, h)].astype(f32)).astype(bf)
        keep1[r % 4] = mine[r % 2, pl.ds(up, h)] + d2d_got[r % 4, pl.ds(up, h)].astype(f32)

    def stage2(r):
        lo, up = pl.multiple_of(q4 * (1 - pb), q4), pl.multiple_of(q4 * pb, q4)
        rs2_out[r % 8] = (keep1[r % 4, pl.ds(lo, q4)] + rs1_got[r % 8, pl.ds(lo, q4)].astype(f32)).astype(bf)
        keep2[r % 4] = keep1[r % 4, pl.ds(up, q4)] + rs1_got[r % 8, pl.ds(up, q4)].astype(f32)

    def quarter(p, q):
        return own + h * p + q4 * q

    def stage3(r):
        t_ref[cut(r, quarter(pa, pb), q4)] = (keep2[r % 4] + rs2_got[r % 8].astype(f32)).astype(bf)

    def spread1(r):
        src = tile(r, quarter(pa, pb), q4)
        remote(src, src, ag_s, ag1_r.at[r], to_b).start()
        remote(src, src, ag_s, ag2a_r.at[r], to_a).start()
        remote(src, src, ag_s, sib_r, sib).start()

    def spread2(r):
        src = tile(r, quarter(pa, 1 - pb), q4)
        remote(src, src, ag_s, ag1_r.at[r], to_b).wait_recv()
        remote(src, src, ag_s, ag2b_r.at[r], to_a).start()
        remote(src, src, ag_s, sib_r, sib).start()

    def spread3(r):
        dst = tile(r, quarter(1 - pa, pb), q4)
        remote(dst, dst, ag_s, ag2a_r.at[r], to_a).wait_recv()
        dst = tile(r, quarter(1 - pa, 1 - pb), q4)
        remote(dst, dst, ag_s, ag2b_r.at[r], to_a).wait_recv()
        src = tile(r, own + h * (1 - pa), h)
        remote(src, src, ag_s, sib_r, sib).start()

    def when(cond, f):
        if cond is True:
            f()
        elif cond is not False:
            pl.when(cond)(f)

    def both(p, q):
        return q if p is True else p & q

    def spread(r):
        s = (r - AG_START) // AG_EVERY

        @pl.when((r >= AG_START) & ((r - AG_START) % AG_EVERY == 0))
        def _():
            spread1(s)

            @pl.when(s >= 1)
            def _():
                spread2(s - 1)

            @pl.when(s >= 2)
            def _():
                spread3(s - 2)

    def round_(r, first=False, compute=True, one=True, two=True, three=True, reuse=True):
        if compute:
            n, j = r // nb, r % nb

            @pl.when((j == 2) & (n + 1 < mats))
            def _():
                for i in range(2):
                    a_copy(n + 1, i).start()

            @pl.when((j == 0) & (n > 0))
            def _():
                for i in range(2):
                    a_copy(n, i).wait()

            g_copy(r).wait()

            @pl.when(r + 2 < rounds)
            def _():
                g_copy(r + 2).start()

            if first:
                @pl.when(r == 0)
                def _():
                    a_side(0, other).wait()
            when((r >= 4) if first else True, lambda: d2d(r - 4).wait_send())
            @pl.when(me >= 0)
            def _():
                d2d_out[r % 4] = dot(r, other).astype(bf)

            d2d(r).start()
            if first:
                @pl.when(r == 0)
                def _():
                    a_side(0, own).wait()

        when(one, lambda: d2d(r - LAG1).wait_recv())
        when(two, lambda: rs1(r - LAG2).wait_recv())
        when(three, lambda: rs2(r - LAG3).wait_recv())
        when(both(one, r - LAG1 >= 8), lambda: rs1(r - LAG1 - 8).wait_send())
        when(both(two, r - LAG2 >= 8), lambda: rs2(r - LAG2 - 8).wait_send())
        when(one, lambda: combine(r - LAG1))
        when(one, lambda: rs1(r - LAG1).start())
        when(two, lambda: stage2(r - LAG2))
        when(two, lambda: rs2(r - LAG2).start())
        if compute:
            mine[r % 2] = dot(r, own)
        when(three, lambda: stage3(r - LAG3))
        spread(r)

    a_side(0, other).start()
    g_copy(0).start()
    a_side(0, own).start()
    g_copy(1).start()

    barrier = pltpu.get_barrier_semaphore()
    for dev in (sib, to_a, to_b):
        pl.semaphore_signal(barrier, inc=1, device_id={"dp": dev}, device_id_type=MESH)
    pl.semaphore_wait(barrier, 3)

    @pl.loop(0, LAG3)
    def _(r):
        round_(r, first=True, one=r >= LAG1, two=r >= LAG2, three=False)

    @pl.loop(LAG3, rounds)
    def _(r):
        round_(r)

    @pl.loop(rounds, rounds + LAG3)
    def _(r):
        round_(r, compute=False, one=r < rounds + LAG1, two=r < rounds + LAG2)

    done = -(-(rounds + LAG3 - AG_START) // AG_EVERY)

    @pl.loop(done, rounds)
    def _(s):
        spread1(s)

    @pl.loop(done - 1, rounds + 1)
    def _(s):
        @pl.when(s < rounds)
        def _():
            spread2(s)

        spread3(s - 1)

    for k in range(4):
        d2d(rounds - 4 + k).wait_send()
    for k in range(8):
        rs1(rounds - 8 + k).wait_send()
        rs2(rounds - 8 + k).wait_send()
    whole = t_ref.at[:, pl.ds(0, d - q4), :]
    remote(whole, whole, ag_s, sib_r, sib).wait_send()
    part = t_ref.at[:, pl.ds(0, half_d), :]
    remote(part, part, ag_s, sib_r, sib).wait_recv()


def put(t_ref, o_ref, sem):
    copies = [pltpu.make_async_copy(t_ref.at[n], o_ref.at[n], sem.at[n]) for n in range(t_ref.shape[0])]
    for copy in copies:
        copy.start()
    for copy in copies:
        copy.wait()


def solution(mesh):
    def step(a, g):
        mats, tokens, d = a.shape[1:]
        ff = g.shape[3]
        rounds = mats * (ff // W)
        bf, f32 = jnp.bfloat16, jnp.float32
        dma = pltpu.SemaphoreType.DMA
        scratch = [
            pltpu.VMEM((2, 2, tokens, d // 2), bf),
            pltpu.VMEM((3, tokens, W), bf),
            pltpu.VMEM((2, d // 2, W), f32),
            pltpu.VMEM((4, d // 2, W), bf),
            pltpu.VMEM((4, d // 2, W), bf),
            pltpu.VMEM((8, d // 4, W), bf),
            pltpu.VMEM((8, d // 4, W), bf),
            pltpu.VMEM((4, d // 4, W), f32),
            pltpu.VMEM((8, d // 8, W), bf),
            pltpu.VMEM((8, d // 8, W), bf),
            pltpu.VMEM((4, d // 8, W), f32),
            dma((2, 2)), dma((3,)), dma((4,)), dma((4,)), dma((8,)), dma((8,)), dma((8,)), dma((8,)),
            dma((rounds,)), dma((rounds,)), dma((rounds,)), dma, dma,
        ]
        t = pl.pallas_call(
            kernel,
            out_shape=pltpu.VMEM((mats, d, ff), bf),
            in_specs=[pl.BlockSpec(memory_space=pl.ANY)] * 2,
            out_specs=pl.BlockSpec(memory_space=pltpu.VMEM),
            scratch_shapes=scratch,
            compiler_params=pltpu.CompilerParams(collective_id=0, has_side_effects=True, vmem_limit_bytes=34 << 20),
            name="sums",
        )(a, g)
        return pl.pallas_call(
            put,
            out_shape=jax.ShapeDtypeStruct((mats, d, ff), bf),
            in_specs=[pl.BlockSpec(memory_space=pltpu.VMEM)],
            out_specs=pl.BlockSpec(memory_space=pl.ANY),
            scratch_shapes=[dma((mats,))],
            compiler_params=pltpu.CompilerParams(vmem_limit_bytes=4 << 20),
            name="put",
        )(t)

    return jax.shard_map(step, mesh=mesh, in_specs=(P(("rep", "dp")), P(("rep", "dp"))), out_specs=P("rep"),
                         check_vma=False)
```

```python
import jax
import jax.numpy as jnp
from jax import lax
from jax.experimental import pallas as pl
from jax.experimental.pallas import tpu as pltpu
from jax.sharding import PartitionSpec as P

MESH = pl.DeviceIdType.MESH
W = 256
LAG1, LAG2, LAG3 = 1, 3, 5
AG_START, AG_SKIP = 5, 2
AGL2, AGL3 = 2, 4


def kernel(a_ref, g_ref, t_ref, a_in, g_in, mine, d2d_out, d2d_got, rs1_out, rs1_got, keep1,
           rs2_out, rs2_got, keep2,
           a_sem, g_sem, d2d_s, d2d_r, rs1_s, rs1_r, rs2_s, rs2_r, ag1_r, ag2a_r, ag2b_r, sib_r, ag_s):
    mats, tokens, d = a_ref.shape[1:]
    ff = g_ref.shape[3]
    nb = ff // W
    rounds = mats * nb
    half_d, h, q4 = d // 2, d // 4, d // 8
    f32, bf = jnp.float32, jnp.bfloat16

    me = lax.axis_index("dp")
    x, y, c = me // 4, (me // 2) % 2, me % 2
    pa = (1 - c) * x + c * y
    pb = (1 - c) * y + c * x
    to_a = me + (1 - c) * (4 - 8 * x) + c * (2 - 4 * y)
    to_b = me + (1 - c) * (2 - 4 * y) + c * (4 - 8 * x)
    sib = me + 1 - 2 * c
    own, other = half_d * c, half_d * (1 - c)

    def remote(src, dst, s, r, dev):
        return pltpu.make_async_remote_copy(src_ref=src, dst_ref=dst, send_sem=s, recv_sem=r,
                                            device_id={"dp": dev}, device_id_type=MESH)

    def cut(r, start, size):
        return r // nb, pl.ds(pl.multiple_of(start, 128), size), pl.ds(pl.multiple_of((r % nb) * W, W), W)

    def tile(r, start, size):
        return t_ref.at[cut(r, start, size)]

    def g_copy(r):
        return pltpu.make_async_copy(g_ref.at[0, r // nb, :, pl.ds(pl.multiple_of((r % nb) * W, W), W)],
                                     g_in.at[r % 3], g_sem.at[r % 3])

    def a_copy(n, i):
        cols = pl.ds(half_d * i, half_d)
        return pltpu.make_async_copy(a_ref.at[0, n, :, cols], a_in.at[n % 2, i], a_sem.at[n % 2, i])

    def a_side(n, side):
        cols = pl.ds(pl.multiple_of(side, half_d), half_d)
        return pltpu.make_async_copy(a_ref.at[0, n, :, cols], a_in.at[n % 2, side // half_d],
                                     a_sem.at[n % 2, side // half_d])

    def d2d(r):
        return remote(d2d_out.at[r % 4], d2d_got.at[r % 4], d2d_s.at[r % 4], d2d_r.at[r % 4], sib)

    def rs1(r):
        return remote(rs1_out.at[r % 8], rs1_got.at[r % 8], rs1_s.at[r % 8], rs1_r.at[r % 8], to_a)

    def rs2(r):
        return remote(rs2_out.at[r % 8], rs2_got.at[r % 8], rs2_s.at[r % 8], rs2_r.at[r % 8], to_b)

    def dot(r, side):
        return lax.dot_general(a_in[(r // nb) % 2, side // half_d], g_in[r % 3],
                               (((0,), (0,)), ((), ())), preferred_element_type=f32)

    def combine(r):
        lo, up = pl.multiple_of(h * (1 - pa), h), pl.multiple_of(h * pa, h)
        rs1_out[r % 8] = (mine[r % 2, pl.ds(lo, h)] + d2d_got[r % 4, pl.ds(lo, h)].astype(f32)).astype(bf)
        keep1[r % 4] = mine[r % 2, pl.ds(up, h)] + d2d_got[r % 4, pl.ds(up, h)].astype(f32)

    def stage2(r):
        lo, up = pl.multiple_of(q4 * (1 - pb), q4), pl.multiple_of(q4 * pb, q4)
        rs2_out[r % 8] = (keep1[r % 4, pl.ds(lo, q4)] + rs1_got[r % 8, pl.ds(lo, q4)].astype(f32)).astype(bf)
        keep2[r % 4] = keep1[r % 4, pl.ds(up, q4)] + rs1_got[r % 8, pl.ds(up, q4)].astype(f32)

    def quarter(p, q):
        return own + h * p + q4 * q

    def stage3(r):
        t_ref[cut(r, quarter(pa, pb), q4)] = (keep2[r % 4] + rs2_got[r % 8].astype(f32)).astype(bf)

    def spread1(r):
        src = tile(r, quarter(pa, pb), q4)
        remote(src, src, ag_s, ag1_r.at[r], to_b).start()
        remote(src, src, ag_s, ag2a_r.at[r], to_a).start()
        remote(src, src, ag_s, sib_r, sib).start()

    def spread2(r):
        src = tile(r, quarter(pa, 1 - pb), q4)
        remote(src, src, ag_s, ag1_r.at[r], to_b).wait_recv()
        remote(src, src, ag_s, ag2b_r.at[r], to_a).start()
        remote(src, src, ag_s, sib_r, sib).start()

    def spread3(r):
        dst = tile(r, quarter(1 - pa, pb), q4)
        remote(dst, dst, ag_s, ag2a_r.at[r], to_a).wait_recv()
        dst = tile(r, quarter(1 - pa, 1 - pb), q4)
        remote(dst, dst, ag_s, ag2b_r.at[r], to_a).wait_recv()
        src = tile(r, own + h * (1 - pa), h)
        remote(src, src, ag_s, sib_r, sib).start()

    def when(cond, f):
        if cond is True:
            f()
        elif cond is not False:
            pl.when(cond)(f)

    def both(p, q):
        return q if p is True else p & q

    def spread(r):
        u = r - AG_START
        s = u - u // AG_SKIP

        @pl.when((u >= 0) & (u % AG_SKIP != AG_SKIP - 1))
        def _():
            spread1(s)

            @pl.when(s >= AGL2)
            def _():
                spread2(s - AGL2)

            @pl.when(s >= AGL3)
            def _():
                spread3(s - AGL3)

    def round_(r, first=False, compute=True, one=True, two=True, three=True, reuse=True):
        if compute:
            n, j = r // nb, r % nb

            @pl.when((j == 2) & (n + 1 < mats))
            def _():
                for i in range(2):
                    a_copy(n + 1, i).start()

            @pl.when((j == 0) & (n > 0))
            def _():
                for i in range(2):
                    a_copy(n, i).wait()

            g_copy(r).wait()

            @pl.when(r + 2 < rounds)
            def _():
                g_copy(r + 2).start()

            if first:
                @pl.when(r == 0)
                def _():
                    a_side(0, other).wait()
            when((r >= 4) if first else True, lambda: d2d(r - 4).wait_send())
            @pl.when(me >= 0)
            def _():
                d2d_out[r % 4] = dot(r, other).astype(bf)

            d2d(r).start()
            if first:
                @pl.when(r == 0)
                def _():
                    a_side(0, own).wait()

        if not first:
            when(one, lambda: d2d(r - LAG1).wait_recv())
        when(two, lambda: rs1(r - LAG2).wait_recv())
        when(three, lambda: rs2(r - LAG3).wait_recv())
        if not first:
            when(both(one, r - LAG1 >= 8), lambda: rs1(r - LAG1 - 8).wait_send())
        when(both(two, r - LAG2 >= 8), lambda: rs2(r - LAG2 - 8).wait_send())
        if not first:
            when(one, lambda: combine(r - LAG1))
            when(one, lambda: rs1(r - LAG1).start())
        when(two, lambda: stage2(r - LAG2))
        when(two, lambda: rs2(r - LAG2).start())
        if compute:
            mine[r % 2] = dot(r, own)
        if first:
            @pl.when(r < LAG3 - LAG1)
            def _():
                d2d(r).wait_recv()
                combine(r)
                rs1(r).start()
        when(three, lambda: stage3(r - LAG3))
        spread(r)

    a_side(0, other).start()
    g_copy(0).start()
    a_side(0, own).start()
    g_copy(1).start()

    barrier = pltpu.get_barrier_semaphore()
    for dev in (sib, to_a, to_b):
        pl.semaphore_signal(barrier, inc=1, device_id={"dp": dev}, device_id_type=MESH)
    pl.semaphore_wait(barrier, 3)

    @pl.loop(0, LAG3)
    def _(r):
        round_(r, first=True, two=r >= LAG2, three=False)

    @pl.loop(LAG3, rounds)
    def _(r):
        round_(r)

    @pl.loop(rounds, rounds + LAG3)
    def _(r):
        round_(r, compute=False, one=r < rounds + LAG1, two=r < rounds + LAG2)

    turns = rounds + LAG3 - AG_START
    done = turns - turns // AG_SKIP

    @pl.loop(done, rounds)
    def _(s):
        spread1(s)

    @pl.loop(done - AGL2, rounds)
    def _(s):
        spread2(s)

    @pl.loop(done - AGL3, rounds)
    def _(s):
        spread3(s)

    for k in range(4):
        d2d(rounds - 4 + k).wait_send()
    for k in range(8):
        rs1(rounds - 8 + k).wait_send()
        rs2(rounds - 8 + k).wait_send()
    whole = t_ref.at[:, pl.ds(0, d - q4), :]
    remote(whole, whole, ag_s, sib_r, sib).wait_send()
    part = t_ref.at[:, pl.ds(0, half_d), :]
    remote(part, part, ag_s, sib_r, sib).wait_recv()


def put(t_ref, o_ref, sem):
    rows = t_ref.shape[1] // 4
    copies = [pltpu.make_async_copy(t_ref.at[n, pl.ds(k * rows, rows)], o_ref.at[n, pl.ds(k * rows, rows)], sem.at[n, k])
              for n in range(t_ref.shape[0]) for k in range(4)]
    for copy in copies:
        copy.start()
    for copy in copies:
        copy.wait()


def solution(mesh):
    def step(a, g):
        mats, tokens, d = a.shape[1:]
        ff = g.shape[3]
        rounds = mats * (ff // W)
        bf, f32 = jnp.bfloat16, jnp.float32
        dma = pltpu.SemaphoreType.DMA
        scratch = [
            pltpu.VMEM((2, 2, tokens, d // 2), bf),
            pltpu.VMEM((3, tokens, W), bf),
            pltpu.VMEM((2, d // 2, W), f32),
            pltpu.VMEM((4, d // 2, W), bf),
            pltpu.VMEM((4, d // 2, W), bf),
            pltpu.VMEM((8, d // 4, W), bf),
            pltpu.VMEM((8, d // 4, W), bf),
            pltpu.VMEM((4, d // 4, W), f32),
            pltpu.VMEM((8, d // 8, W), bf),
            pltpu.VMEM((8, d // 8, W), bf),
            pltpu.VMEM((4, d // 8, W), f32),
            dma((2, 2)), dma((3,)), dma((4,)), dma((4,)), dma((8,)), dma((8,)), dma((8,)), dma((8,)),
            dma((rounds,)), dma((rounds,)), dma((rounds,)), dma, dma,
        ]
        t = pl.pallas_call(
            kernel,
            out_shape=pltpu.VMEM((mats, d, ff), bf),
            in_specs=[pl.BlockSpec(memory_space=pl.ANY)] * 2,
            out_specs=pl.BlockSpec(memory_space=pltpu.VMEM),
            scratch_shapes=scratch,
            compiler_params=pltpu.CompilerParams(collective_id=0, has_side_effects=True, vmem_limit_bytes=34 << 20),
            name="sums",
        )(a, g)
        return pl.pallas_call(
            put,
            out_shape=jax.ShapeDtypeStruct((mats, d, ff), bf),
            in_specs=[pl.BlockSpec(memory_space=pltpu.VMEM)],
            out_specs=pl.BlockSpec(memory_space=pl.ANY),
            scratch_shapes=[dma((mats, 4))],
            compiler_params=pltpu.CompilerParams(vmem_limit_bytes=4 << 20),
            name="put",
        )(t)

    return jax.shard_map(step, mesh=mesh, in_specs=(P(("rep", "dp")), P(("rep", "dp"))), out_specs=P("rep"),
                         check_vma=False)
```

```python
import jax
import jax.numpy as jnp
from jax import lax
from jax.experimental import pallas as pl
from jax.experimental.pallas import tpu as pltpu
from jax.sharding import PartitionSpec as P

MESH = pl.DeviceIdType.MESH
W = 256
RAMP, LAG2, LAG3 = 8, 3, 5
AG_START, AG_SKIP = 4, 4
AGL2, AGL3 = 2, 4


def kernel(a_ref, g_ref, t_ref, a_in, g_in, mine, d2d_out, d2d_got, rs1_out, rs1_got, keep1,
           rs2_out, rs2_got, keep2,
           a_sem, g_sem, d2d_s, d2d_r, rs1_s, rs1_r, rs2_s, rs2_r, ag1_r, ag2a_r, ag2b_r, sib_r, ag_s):
    mats, tokens, d = a_ref.shape[1:]
    ff = g_ref.shape[3]
    nb = ff // W
    rounds = mats * nb
    half_d, h, q4 = d // 2, d // 4, d // 8
    f32, bf = jnp.float32, jnp.bfloat16

    me = lax.axis_index("dp")
    x, y, c = me // 4, (me // 2) % 2, me % 2
    pa = (1 - c) * x + c * y
    pb = (1 - c) * y + c * x
    to_a = me + (1 - c) * (4 - 8 * x) + c * (2 - 4 * y)
    to_b = me + (1 - c) * (2 - 4 * y) + c * (4 - 8 * x)
    sib = me + 1 - 2 * c
    own, other = half_d * c, half_d * (1 - c)

    def remote(src, dst, s, r, dev):
        return pltpu.make_async_remote_copy(src_ref=src, dst_ref=dst, send_sem=s, recv_sem=r,
                                            device_id={"dp": dev}, device_id_type=MESH)

    def cut(r, start, size):
        return r // nb, pl.ds(pl.multiple_of(start, 128), size), pl.ds(pl.multiple_of((r % nb) * W, W), W)

    def tile(r, start, size):
        return t_ref.at[cut(r, start, size)]

    def g_copy(r):
        return pltpu.make_async_copy(g_ref.at[0, r // nb, :, pl.ds(pl.multiple_of((r % nb) * W, W), W)],
                                     g_in.at[r % 3], g_sem.at[r % 3])

    def a_copy(n, i):
        cols = pl.ds(half_d * i, half_d)
        return pltpu.make_async_copy(a_ref.at[0, n, :, cols], a_in.at[n % 2, i], a_sem.at[n % 2, i])

    def a_side(n, side):
        cols = pl.ds(pl.multiple_of(side, half_d), half_d)
        return pltpu.make_async_copy(a_ref.at[0, n, :, cols], a_in.at[n % 2, side // half_d],
                                     a_sem.at[n % 2, side // half_d])

    def d2d(r):
        return remote(d2d_out.at[r % 4], d2d_got.at[r % 4], d2d_s.at[r % 4], d2d_r.at[r % 4], sib)

    def rs1(r):
        return remote(rs1_out.at[r % 8], rs1_got.at[r % 8], rs1_s.at[r % 8], rs1_r.at[r % 8], to_a)

    def rs2(r):
        return remote(rs2_out.at[r % 8], rs2_got.at[r % 8], rs2_s.at[r % 8], rs2_r.at[r % 8], to_b)

    def dot(r, side):
        return lax.dot_general(a_in[(r // nb) % 2, side // half_d], g_in[r % 3],
                               (((0,), (0,)), ((), ())), preferred_element_type=f32)

    def combine(r):
        lo, up = pl.multiple_of(h * (1 - pa), h), pl.multiple_of(h * pa, h)
        rs1_out[r % 8] = (mine[r % 2, pl.ds(lo, h)] + d2d_got[r % 4, pl.ds(lo, h)].astype(f32)).astype(bf)
        keep1[r % 4] = mine[r % 2, pl.ds(up, h)] + d2d_got[r % 4, pl.ds(up, h)].astype(f32)

    def stage2(r):
        lo, up = pl.multiple_of(q4 * (1 - pb), q4), pl.multiple_of(q4 * pb, q4)
        rs2_out[r % 8] = (keep1[r % 4, pl.ds(lo, q4)] + rs1_got[r % 8, pl.ds(lo, q4)].astype(f32)).astype(bf)
        keep2[r % 4] = keep1[r % 4, pl.ds(up, q4)] + rs1_got[r % 8, pl.ds(up, q4)].astype(f32)

    def quarter(p, q):
        return own + h * p + q4 * q

    def stage3(r):
        t_ref[cut(r, quarter(pa, pb), q4)] = (keep2[r % 4] + rs2_got[r % 8].astype(f32)).astype(bf)

    def spread1(r):
        src = tile(r, quarter(pa, pb), q4)
        remote(src, src, ag_s, ag1_r.at[r], to_b).start()
        remote(src, src, ag_s, ag2a_r.at[r], to_a).start()
        remote(src, src, ag_s, sib_r, sib).start()

    def spread2(r):
        src = tile(r, quarter(pa, 1 - pb), q4)
        remote(src, src, ag_s, ag1_r.at[r], to_b).wait_recv()
        remote(src, src, ag_s, ag2b_r.at[r], to_a).start()
        remote(src, src, ag_s, sib_r, sib).start()

    def spread3(r):
        dst = tile(r, quarter(1 - pa, pb), q4)
        remote(dst, dst, ag_s, ag2a_r.at[r], to_a).wait_recv()
        dst = tile(r, quarter(1 - pa, 1 - pb), q4)
        remote(dst, dst, ag_s, ag2b_r.at[r], to_a).wait_recv()
        src = tile(r, own + h * (1 - pa), h)
        remote(src, src, ag_s, sib_r, sib).start()

    def when(cond, f):
        if cond is True:
            f()
        elif cond is not False:
            pl.when(cond)(f)

    def both(p, q):
        return q if p is True else p & q

    def spread(r):
        u = r - AG_START
        s = u - u // AG_SKIP

        @pl.when((u >= 0) & (u % AG_SKIP != AG_SKIP - 1))
        def _():
            spread1(s)

            @pl.when(s >= AGL2)
            def _():
                spread2(s - AGL2)

            @pl.when(s >= AGL3)
            def _():
                spread3(s - AGL3)

    def round_(r, lag2, lag3, first=False, compute=True, two=True, three=True):
        if compute:
            n, j = r // nb, r % nb

            @pl.when((j == 2) & (n + 1 < mats))
            def _():
                for i in range(2):
                    a_copy(n + 1, i).start()

            @pl.when((j == 0) & (n > 0))
            def _():
                for i in range(2):
                    a_copy(n, i).wait()

            g_copy(r).wait()

            @pl.when(r + 2 < rounds)
            def _():
                g_copy(r + 2).start()

            if first:
                @pl.when(r == 0)
                def _():
                    a_side(0, other).wait()
            when((r >= 4) if first else True, lambda: d2d(r - 4).wait_send())
            @pl.when(me >= 0)
            def _():
                d2d_out[r % 4] = dot(r, other).astype(bf)

            d2d(r).start()
            if first:
                @pl.when(r == 0)
                def _():
                    a_side(0, own).wait()

        when(two, lambda: rs1(r - lag2).wait_recv())
        when(three, lambda: rs2(r - lag3).wait_recv())
        when(both(two, r - lag2 >= 8), lambda: rs2(r - lag2 - 8).wait_send())
        when(two, lambda: stage2(r - lag2))
        when(two, lambda: rs2(r - lag2).start())
        if compute:
            mine[r % 2] = dot(r, own)
        when(three, lambda: stage3(r - lag3))
        if compute:
            when(r >= 8, lambda: rs1(r - 8).wait_send())
            d2d(r).wait_recv()
            combine(r)
            rs1(r).start()
        spread(r)

    a_side(0, other).start()
    g_copy(0).start()

    barrier = pltpu.get_barrier_semaphore()
    for dev in (sib, to_a, to_b):
        pl.semaphore_signal(barrier, inc=1, device_id={"dp": dev}, device_id_type=MESH)
    pl.semaphore_wait(barrier, 3)

    a_side(0, own).start()
    g_copy(1).start()

    @pl.loop(0, RAMP)
    def _(r):
        round_(r, 2, 3, first=True, two=(r >= 2) & (r - 2 < RAMP - LAG2), three=(r >= 3) & (r - 3 < RAMP - LAG3))

    @pl.loop(RAMP, rounds)
    def _(r):
        round_(r, LAG2, LAG3)

    @pl.loop(rounds, rounds + LAG3)
    def _(r):
        round_(r, LAG2, LAG3, compute=False, two=r < rounds + LAG2)

    turns = rounds + LAG3 - AG_START
    done = turns - turns // AG_SKIP

    @pl.loop(done, rounds)
    def _(s):
        spread1(s)

    @pl.loop(done - AGL2, rounds)
    def _(s):
        spread2(s)

    @pl.loop(done - AGL3, rounds)
    def _(s):
        spread3(s)

    for k in range(4):
        d2d(rounds - 4 + k).wait_send()
    for k in range(8):
        rs1(rounds - 8 + k).wait_send()
        rs2(rounds - 8 + k).wait_send()
    whole = t_ref.at[:, pl.ds(0, d - q4), :]
    remote(whole, whole, ag_s, sib_r, sib).wait_send()
    part = t_ref.at[:, pl.ds(0, half_d), :]
    remote(part, part, ag_s, sib_r, sib).wait_recv()


def put(t_ref, o_ref, sem):
    rows = t_ref.shape[1] // 4
    copies = [pltpu.make_async_copy(t_ref.at[n, pl.ds(k * rows, rows)], o_ref.at[n, pl.ds(k * rows, rows)], sem.at[n, k])
              for n in range(t_ref.shape[0]) for k in range(4)]
    for copy in copies:
        copy.start()
    for copy in copies:
        copy.wait()


def solution(mesh):
    def step(a, g):
        mats, tokens, d = a.shape[1:]
        ff = g.shape[3]
        rounds = mats * (ff // W)
        bf, f32 = jnp.bfloat16, jnp.float32
        dma = pltpu.SemaphoreType.DMA
        scratch = [
            pltpu.VMEM((2, 2, tokens, d // 2), bf),
            pltpu.VMEM((3, tokens, W), bf),
            pltpu.VMEM((2, d // 2, W), f32),
            pltpu.VMEM((4, d // 2, W), bf),
            pltpu.VMEM((4, d // 2, W), bf),
            pltpu.VMEM((8, d // 4, W), bf),
            pltpu.VMEM((8, d // 4, W), bf),
            pltpu.VMEM((4, d // 4, W), f32),
            pltpu.VMEM((8, d // 8, W), bf),
            pltpu.VMEM((8, d // 8, W), bf),
            pltpu.VMEM((4, d // 8, W), f32),
            dma((2, 2)), dma((3,)), dma((4,)), dma((4,)), dma((8,)), dma((8,)), dma((8,)), dma((8,)),
            dma((rounds,)), dma((rounds,)), dma((rounds,)), dma, dma,
        ]
        t = pl.pallas_call(
            kernel,
            out_shape=pltpu.VMEM((mats, d, ff), bf),
            in_specs=[pl.BlockSpec(memory_space=pl.ANY)] * 2,
            out_specs=pl.BlockSpec(memory_space=pltpu.VMEM),
            scratch_shapes=scratch,
            compiler_params=pltpu.CompilerParams(collective_id=0, has_side_effects=True, vmem_limit_bytes=34 << 20),
            name="sums",
        )(a, g)
        return pl.pallas_call(
            put,
            out_shape=jax.ShapeDtypeStruct((mats, d, ff), bf),
            in_specs=[pl.BlockSpec(memory_space=pltpu.VMEM)],
            out_specs=pl.BlockSpec(memory_space=pl.ANY),
            scratch_shapes=[dma((mats, 4))],
            compiler_params=pltpu.CompilerParams(vmem_limit_bytes=4 << 20),
            name="put",
        )(t)

    return jax.shard_map(step, mesh=mesh, in_specs=(P(("rep", "dp")), P(("rep", "dp"))), out_specs=P("rep"),
                         check_vma=False)
```

```python
import jax
import jax.numpy as jnp
from jax import lax
from jax.experimental import pallas as pl
from jax.experimental.pallas import tpu as pltpu
from jax.sharding import PartitionSpec as P

MESH = pl.DeviceIdType.MESH
W = 256
RAMP, LAG2, LAG3 = 8, 3, 5
AG_START, AG_SKIP = 4, 4
AGL2, AGL3 = 2, 4


def kernel(a_ref, g_ref, t_ref, a_in, g_in, mine, d2d_out, d2d_got, rs1_out, rs1_got, keep1,
           rs2_out, rs2_got, keep2,
           h_sem, a_sem, g_sem, d2d_s, d2d_r, rs1_s, rs1_r, rs2_s, rs2_r, ag1_r, ag2a_r, ag2b_r, sib_r, ag_s):
    mats, tokens, d = a_ref.shape[1:]
    ff = g_ref.shape[3]
    nb = ff // W
    rounds = mats * nb
    half_d, h, q4 = d // 2, d // 4, d // 8
    f32, bf = jnp.float32, jnp.bfloat16

    me = lax.axis_index("dp")
    x, y, c = me // 4, (me // 2) % 2, me % 2
    pa = (1 - c) * x + c * y
    pb = (1 - c) * y + c * x
    to_a = me + (1 - c) * (4 - 8 * x) + c * (2 - 4 * y)
    to_b = me + (1 - c) * (2 - 4 * y) + c * (4 - 8 * x)
    sib = me + 1 - 2 * c
    own, other = half_d * c, half_d * (1 - c)

    def remote(src, dst, s, r, dev):
        return pltpu.make_async_remote_copy(src_ref=src, dst_ref=dst, send_sem=s, recv_sem=r,
                                            device_id={"dp": dev}, device_id_type=MESH)

    def cut(r, start, size):
        return r // nb, pl.ds(pl.multiple_of(start, 128), size), pl.ds(pl.multiple_of((r % nb) * W, W), W)

    def tile(r, start, size):
        return t_ref.at[cut(r, start, size)]

    def g_copy(r):
        return pltpu.make_async_copy(g_ref.at[0, r // nb, :, pl.ds(pl.multiple_of((r % nb) * W, W), W)],
                                     g_in.at[r % 3], g_sem.at[r % 3])

    def a_copy(n, i):
        cols = pl.ds(half_d * i, half_d)
        return pltpu.make_async_copy(a_ref.at[0, n, :, cols], a_in.at[n % 2, i], a_sem.at[n % 2, i])

    def a_side(n, side):
        cols = pl.ds(pl.multiple_of(side, half_d), half_d)
        return pltpu.make_async_copy(a_ref.at[0, n, :, cols], a_in.at[n % 2, side // half_d],
                                     a_sem.at[n % 2, side // half_d])

    def d2d(r):
        return remote(d2d_out.at[r % 4], d2d_got.at[r % 4], d2d_s.at[r % 4], d2d_r.at[r % 4], sib)

    def rs1(r):
        return remote(rs1_out.at[r % 8], rs1_got.at[r % 8], rs1_s.at[r % 8], rs1_r.at[r % 8], to_a)

    def rs2(r):
        return remote(rs2_out.at[r % 8], rs2_got.at[r % 8], rs2_s.at[r % 8], rs2_r.at[r % 8], to_b)

    def dot(r, side):
        return lax.dot_general(a_in[(r // nb) % 2, side // half_d], g_in[r % 3],
                               (((0,), (0,)), ((), ())), preferred_element_type=f32)

    def head(k):
        rows = pl.ds(tokens // 2 * k, tokens // 2)
        cols = pl.ds(pl.multiple_of(other, half_d), half_d)
        return (pltpu.make_async_copy(a_ref.at[0, 0, rows, cols], a_in.at[0, other // half_d, rows], h_sem.at[k, 0]),
                pltpu.make_async_copy(g_ref.at[0, 0, rows, pl.ds(0, W)], g_in.at[0, rows], h_sem.at[k, 1]))

    def head_dot(k):
        for copy in head(k):
            copy.wait()
        rows = pl.ds(tokens // 2 * k, tokens // 2)
        return lax.dot_general(a_in[0, other // half_d, rows], g_in[0, rows], (((0,), (0,)), ((), ())),
                               preferred_element_type=f32)

    def combine(r):
        lo, up = pl.multiple_of(h * (1 - pa), h), pl.multiple_of(h * pa, h)
        rs1_out[r % 8] = (mine[r % 2, pl.ds(lo, h)] + d2d_got[r % 4, pl.ds(lo, h)].astype(f32)).astype(bf)
        keep1[r % 4] = mine[r % 2, pl.ds(up, h)] + d2d_got[r % 4, pl.ds(up, h)].astype(f32)

    def stage2(r):
        lo, up = pl.multiple_of(q4 * (1 - pb), q4), pl.multiple_of(q4 * pb, q4)
        rs2_out[r % 8] = (keep1[r % 4, pl.ds(lo, q4)] + rs1_got[r % 8, pl.ds(lo, q4)].astype(f32)).astype(bf)
        keep2[r % 4] = keep1[r % 4, pl.ds(up, q4)] + rs1_got[r % 8, pl.ds(up, q4)].astype(f32)

    def quarter(p, q):
        return own + h * p + q4 * q

    def stage3(r):
        t_ref[cut(r, quarter(pa, pb), q4)] = (keep2[r % 4] + rs2_got[r % 8].astype(f32)).astype(bf)

    def spread1(r):
        src = tile(r, quarter(pa, pb), q4)
        remote(src, src, ag_s, ag1_r.at[r], to_b).start()
        remote(src, src, ag_s, ag2a_r.at[r], to_a).start()
        remote(src, src, ag_s, sib_r, sib).start()

    def spread2(r):
        src = tile(r, quarter(pa, 1 - pb), q4)
        remote(src, src, ag_s, ag1_r.at[r], to_b).wait_recv()
        remote(src, src, ag_s, ag2b_r.at[r], to_a).start()
        remote(src, src, ag_s, sib_r, sib).start()

    def spread3(r):
        dst = tile(r, quarter(1 - pa, pb), q4)
        remote(dst, dst, ag_s, ag2a_r.at[r], to_a).wait_recv()
        dst = tile(r, quarter(1 - pa, 1 - pb), q4)
        remote(dst, dst, ag_s, ag2b_r.at[r], to_a).wait_recv()
        src = tile(r, own + h * (1 - pa), h)
        remote(src, src, ag_s, sib_r, sib).start()

    def when(cond, f):
        if cond is True:
            f()
        elif cond is not False:
            pl.when(cond)(f)

    def both(p, q):
        return q if p is True else p & q

    def spread(r):
        u = r - AG_START
        s = u - u // AG_SKIP

        @pl.when((u >= 0) & (u % AG_SKIP != AG_SKIP - 1))
        def _():
            spread1(s)

            @pl.when(s >= AGL2)
            def _():
                spread2(s - AGL2)

            @pl.when(s >= AGL3)
            def _():
                spread3(s - AGL3)

    def round_(r, lag2, lag3, first=False, compute=True, two=True, three=True):
        if compute:
            n, j = r // nb, r % nb

            @pl.when((j == 2) & (n + 1 < mats))
            def _():
                for i in range(2):
                    a_copy(n + 1, i).start()

            @pl.when((j == 0) & (n > 0))
            def _():
                for i in range(2):
                    a_copy(n, i).wait()

            when(r > 0 if first else True, lambda: g_copy(r).wait())

            @pl.when(r + 2 < rounds)
            def _():
                g_copy(r + 2).start()

            when((r >= 4) if first else True, lambda: d2d(r - 4).wait_send())
            if first:
                @pl.when(r == 0)
                def _():
                    mine[1] = head_dot(0)

                @pl.when((r == 0) & (me >= 0))
                def _():
                    d2d_out[0] = (mine[1] + head_dot(1)).astype(bf)

            @pl.when((r > 0) if first else (me >= 0))
            def _():
                d2d_out[r % 4] = dot(r, other).astype(bf)

            d2d(r).start()
            if first:
                @pl.when(r == 0)
                def _():
                    a_side(0, own).wait()

        when(two, lambda: rs1(r - lag2).wait_recv())
        when(three, lambda: rs2(r - lag3).wait_recv())
        when(both(two, r - lag2 >= 8), lambda: rs2(r - lag2 - 8).wait_send())
        when(two, lambda: stage2(r - lag2))
        when(two, lambda: rs2(r - lag2).start())
        if compute:
            mine[r % 2] = dot(r, own)
        when(three, lambda: stage3(r - lag3))
        if compute:
            when(r >= 8, lambda: rs1(r - 8).wait_send())
            d2d(r).wait_recv()
            combine(r)
            rs1(r).start()
        spread(r)

    for k in range(2):
        for copy in head(k):
            copy.start()

    barrier = pltpu.get_barrier_semaphore()
    for dev in (sib, to_a, to_b):
        pl.semaphore_signal(barrier, inc=1, device_id={"dp": dev}, device_id_type=MESH)
    pl.semaphore_wait(barrier, 3)

    a_side(0, own).start()
    g_copy(1).start()

    @pl.loop(0, RAMP)
    def _(r):
        round_(r, 2, 3, first=True, two=(r >= 2) & (r - 2 < RAMP - LAG2), three=(r >= 3) & (r - 3 < RAMP - LAG3))

    @pl.loop(RAMP, rounds)
    def _(r):
        round_(r, LAG2, LAG3)

    @pl.loop(rounds, rounds + LAG3)
    def _(r):
        round_(r, LAG2, LAG3, compute=False, two=r < rounds + LAG2)

    turns = rounds + LAG3 - AG_START
    done = turns - turns // AG_SKIP

    @pl.loop(done, rounds)
    def _(s):
        spread1(s)

    @pl.loop(done - AGL2, rounds)
    def _(s):
        spread2(s)

    @pl.loop(done - AGL3, rounds)
    def _(s):
        spread3(s)

    for k in range(4):
        d2d(rounds - 4 + k).wait_send()
    for k in range(8):
        rs1(rounds - 8 + k).wait_send()
        rs2(rounds - 8 + k).wait_send()
    whole = t_ref.at[:, pl.ds(0, d - q4), :]
    remote(whole, whole, ag_s, sib_r, sib).wait_send()
    part = t_ref.at[:, pl.ds(0, half_d), :]
    remote(part, part, ag_s, sib_r, sib).wait_recv()


def put(t_ref, o_ref, sem):
    rows = t_ref.shape[1] // 4
    copies = [pltpu.make_async_copy(t_ref.at[n, pl.ds(k * rows, rows)], o_ref.at[n, pl.ds(k * rows, rows)], sem.at[n, k])
              for n in range(t_ref.shape[0]) for k in range(4)]
    for copy in copies:
        copy.start()
    for copy in copies:
        copy.wait()


def solution(mesh):
    def step(a, g):
        mats, tokens, d = a.shape[1:]
        ff = g.shape[3]
        rounds = mats * (ff // W)
        bf, f32 = jnp.bfloat16, jnp.float32
        dma = pltpu.SemaphoreType.DMA
        scratch = [
            pltpu.VMEM((2, 2, tokens, d // 2), bf),
            pltpu.VMEM((3, tokens, W), bf),
            pltpu.VMEM((2, d // 2, W), f32),
            pltpu.VMEM((4, d // 2, W), bf),
            pltpu.VMEM((4, d // 2, W), bf),
            pltpu.VMEM((8, d // 4, W), bf),
            pltpu.VMEM((8, d // 4, W), bf),
            pltpu.VMEM((4, d // 4, W), f32),
            pltpu.VMEM((8, d // 8, W), bf),
            pltpu.VMEM((8, d // 8, W), bf),
            pltpu.VMEM((4, d // 8, W), f32),
            dma((2, 2)), dma((2, 2)), dma((3,)), dma((4,)), dma((4,)), dma((8,)), dma((8,)), dma((8,)), dma((8,)),
            dma((rounds,)), dma((rounds,)), dma((rounds,)), dma, dma,
        ]
        t = pl.pallas_call(
            kernel,
            out_shape=pltpu.VMEM((mats, d, ff), bf),
            in_specs=[pl.BlockSpec(memory_space=pl.ANY)] * 2,
            out_specs=pl.BlockSpec(memory_space=pltpu.VMEM),
            scratch_shapes=scratch,
            compiler_params=pltpu.CompilerParams(collective_id=0, has_side_effects=True, vmem_limit_bytes=34 << 20),
            name="sums",
        )(a, g)
        return pl.pallas_call(
            put,
            out_shape=jax.ShapeDtypeStruct((mats, d, ff), bf),
            in_specs=[pl.BlockSpec(memory_space=pltpu.VMEM)],
            out_specs=pl.BlockSpec(memory_space=pl.ANY),
            scratch_shapes=[dma((mats, 4))],
            compiler_params=pltpu.CompilerParams(vmem_limit_bytes=4 << 20),
            name="put",
        )(t)

    return jax.shard_map(step, mesh=mesh, in_specs=(P(("rep", "dp")), P(("rep", "dp"))), out_specs=P("rep"),
                         check_vma=False)
```
